32 devices in a mesh: group: 4 (over z), member: 8 (over y, x, core).
Axes of the slice: x: 2, y: 2, z: 4, core: 2. Of those that a mesh axis runs over, the one named last changes fastest.
Arguments:
- hidden: bfloat16 [6144, 2048], P('group'), may hold values from -6 to 6
- token_slab: int32 [6144, 1], P(('group', 'member')), may hold values from 0 to 31; in each aligned block of 192 rows (0 to 191, 192 to 383, ...) at most 12 rows name the same one
- token_row: int32 [6144], P(('group', 'member')), may hold values from 0 to 8191
- slab_owner: int32 [32], replicated, may hold values from 0 to 31, each once
- ple_table: bfloat16 [262144, 256], P(('group', 'member')), may hold values from -0.375 to 0.375
- norm_gains: float32 [1, 3, 2048], replicated, may hold values from 0.1 to 1.9
- w_gate: bfloat16 [1, 2048, 8192], P(None, None, 'member'), may hold values from -0.125 to 0.125
- w_up: bfloat16 [1, 2048, 8192], P(None, None, 'member'), may hold values from -0.125 to 0.125
- w_down: bfloat16 [1, 8192, 2048], P(None, 'member'), may hold values from -0.0625 to 0.0625
- ple_gate: bfloat16 [1, 2048, 256], P(None, None, 'member'), may hold values from -0.125 to 0.125
- ple_proj: bfloat16 [1, 256, 2048], P(None, 'member'), may hold values from -0.375 to 0.375
Outputs:
- hidden_out: bfloat16 [6144, 2048], P('group')
The draws below stay inside these ranges and needn't reach their ends.
Inputs may be any that keep to these rules, and one draw needn't show every extreme that they name: Within the 192 tokens of one device (aligned blocks of token_slab), no slab is named by more than 12 tokens. Each number appears once: slab s is stored in rows slab_owner[s] * 8192 to slab_owner[s] * 8192 + 8191 of ple_table.
All inputs are finite; a program needn't handle non-finite values.
Results may differ from the reference program's by a relative error of at most 0.0061.
Values may be sent and summed in bfloat16 or wider, within the bound.
No kernel may reach another device: no remote copies, remote signals or barrier semaphores. Data moves between devices by JAX's collectives and lax.ppermute only.
A program may use at most 128 MiB of HBM per device.

```python
import math
import jax
import jax.numpy as jnp
import numpy as np
from jax import lax

D = 2048
FF = 8192
PLE = 256
VOCAB = 262144
LAYERS = 1
SEQS = 6144
TOK_DEV = 192
CAP = 12
SLAB = 8192
PLEW = 256
DEVICES = 32


def plant(array, stream_key, low, top_value):
    longest = array.shape.index(max(array.shape))
    spots = []
    for shift in (0, 1):
        where = [jax.random.randint(jax.random.fold_in(stream_key, axis), (), 0, length) for axis, length in enumerate(array.shape)]
        where[longest] = (where[longest] + shift) % array.shape[longest]
        spots.append(tuple(where))
    return array.at[spots[0]].set(low).at[spots[1]].set(top_value)


def steps_of(rng, shape, cuts, smallest, top_value):
    def one(position, shards_of):
        draws = jax.random.uniform(jax.random.fold_in(jax.random.fold_in(rng, 6), position), (shards_of,), jnp.float32, smallest / len(cuts), top_value / len(cuts))
        return jnp.repeat(jnp.exp(draws), shape[position] // shards_of).reshape((-1,) + (1,) * (len(shape) - position - 1))

    factor_of = one(*cuts[0])
    for cut in cuts[1:]:
        factor_of = factor_of * one(*cut)
    return factor_of


def rank_table(amount, slope):
    loads = [(1 << 20) // math.isqrt(rank ** slope) + 1 for rank in range(1, amount + 1)]
    deviation = 1 + sum(loads) // (1 << 30)
    return np.cumsum(np.array([max(1, weight // deviation) for weight in loads]))


def ranked_ids(rng, extent, amount, lean):
    grid = rank_table(amount, lean)
    ticket = jax.random.randint(jax.random.fold_in(rng, 1), extent, 0, int(grid[amount - 1]))
    rank = jnp.searchsorted(jnp.asarray(grid, jnp.int32), ticket, side="right")
    return jax.random.permutation(jax.random.fold_in(rng, 2), amount)[rank].astype(jnp.int32)


def deal_out(stream_key, own, number, rows, number_of, top, bound, slope):
    ranking = jax.random.permutation(stream_key, number_of)
    crowded, usual = shares(number_of, rows * top, bound, slope, True), shares(number_of, rows * top, bound, slope, False)
    places = jnp.arange(number_of)

    def named(tallies, rotation):
        used = int((tallies > 0).sum())
        fixed = max(1, used // 4)
        passed = fixed + (places - fixed + rotation * (used - fixed)) % max(1, number_of - fixed)
        return jnp.zeros((number_of,), jnp.int32).at[ranking[jnp.where(places < fixed, places, passed)]].set(jnp.asarray(tallies, jnp.int32))

    tallies = jnp.where(number % 4 == 0, named(crowded, number // 4), named(usual, number - number // 4 - 1))
    mixed = jax.random.permutation(jax.random.fold_in(own, 3), number_of)
    donor, receiver = mixed[0:number_of // 2 * 2:2], mixed[1:number_of // 2 * 2:2]
    room = jnp.minimum(tallies[donor] - 1, bound - tallies[receiver]) // 2
    room = jnp.where((donor == ranking[0]) | (receiver == ranking[0]) | (tallies[receiver] == 0), 0, jnp.maximum(room, 0))
    passed = jax.random.randint(jax.random.fold_in(own, 4), (number_of // 2,), 0, 1 << 20) % (room + 1)
    tallies = tallies.at[donor].add(-passed).at[receiver].add(passed)
    labels = jnp.searchsorted(jnp.cumsum(tallies), jnp.arange(rows * top), side="right").astype(jnp.int32)
    table = labels.reshape(top, rows).T
    table = table[jax.random.permutation(jax.random.fold_in(own, 1), rows)]
    rotation = jax.random.randint(jax.random.fold_in(own, 2), (rows, 1), 0, top)
    return jnp.take_along_axis(table, (jnp.arange(top)[None, :] + rotation) % top, axis=1)


def shares(count, total, limit, slope, full):
    loads = [(1 << 20) // math.isqrt(rank ** slope) + 1 for rank in range(1, count + 1)]
    largest = limit if full else min(limit, max(-(-total // count), total * loads[0] // sum(loads)))
    least = 1 if total - largest >= count - 1 else 0
    given, spare = [largest] + [least] * (count - 1), total - largest - least * (count - 1)
    while spare > 0:
        free = [i for i in range(1, count) if given[i] < largest] or [i for i in range(1, count) if given[i] < limit]
        mass, budget = sum([loads[i] for i in free]), spare
        for i in free:
            addition = min(limit - given[i], max(1, budget * loads[i] // mass), spare)
            given[i] = given[i] + addition
            spare = spare - addition
    return np.array(given)


def noise(own_key, shape, width, bound, pieces=(), held_as=jnp.bfloat16):
    gain = steps_of(own_key, shape, pieces, -0.22, 0.18) if pieces else 1.0
    drawn = jax.random.normal(own_key, shape, jnp.float32) * width * gain
    return jnp.minimum(jnp.maximum(drawn, -bound), bound).astype(held_as)


def setup_inputs(seed: int = 0) -> dict:
    streams_of = jax.random.split(jax.random.key(seed), 12)
    hidden = noise(streams_of[0], (SEQS, D), 1.0, 6.0, ((0, 4),))
    token_slab_keys = jax.random.split(jax.random.fold_in(streams_of[1], 1), SEQS // TOK_DEV)
    token_slab_turns = jax.random.permutation(jax.random.fold_in(streams_of[1], 3), SEQS // TOK_DEV)
    token_slab = jax.vmap(lambda own, number: deal_out(jax.random.fold_in(streams_of[1], 2), own, number, TOK_DEV, DEVICES, 1, CAP, 2))(token_slab_keys, token_slab_turns).reshape((SEQS, 1))
    token_row = plant(ranked_ids(streams_of[2], (SEQS,), SLAB, 2), jax.random.fold_in(streams_of[2], 3), 0, SLAB - 1).astype(jnp.int32)
    slab_owner = jax.random.permutation(streams_of[3], DEVICES).astype(jnp.int32)
    ple_table = noise(streams_of[4], (VOCAB, PLEW), 0.0625, 0.375, ((0, 32),))
    norm_gains = jnp.clip(1.0 + 0.18 * jax.random.normal(streams_of[5], (LAYERS, 3, D), jnp.float32), 0.1, 1.9)
    w_gate = noise(streams_of[6], (LAYERS, D, FF), D ** -0.5, 0.125, ((2, 8),))
    w_up = noise(streams_of[7], (LAYERS, D, FF), D ** -0.5, 0.125, ((2, 8),))
    w_down = noise(streams_of[8], (LAYERS, FF, D), FF ** -0.5, 0.0625, ((1, 8),))
    ple_gate = noise(streams_of[9], (LAYERS, D, PLE), D ** -0.5, 0.125, ((2, 8),))
    ple_proj = noise(streams_of[10], (LAYERS, PLE, D), PLE ** -0.5, 0.375, ((1, 8),))
    return {"hidden": hidden, "token_slab": token_slab, "token_row": token_row, "slab_owner": slab_owner, "ple_table": ple_table, "norm_gains": norm_gains, "w_gate": w_gate, "w_up": w_up, "w_down": w_down, "ple_gate": ple_gate, "ple_proj": ple_proj}


epsilon = 1e-06

def norm_rows(values, scales):
    return values * lax.rsqrt(lax.optimization_barrier(jnp.mean(values * values, axis=-1, keepdims=True)) + epsilon) * scales

def reference(hidden, token_slab, token_row, slab_owner, ple_table, norm_gains, w_gate, w_up, w_down, ple_gate, ple_proj):
    store_index = (slab_owner[token_slab[:, 0]] * SLAB + token_row).astype(jnp.int32)
    looked = jnp.take(ple_table, store_index, axis=0)
    ple_part = looked.astype(jnp.float32).reshape(SEQS, LAYERS, PLE) * PLE ** 0.5
    current = hidden.astype(jnp.float32)
    for layer_at in range(LAYERS):
        normed = norm_rows(current, norm_gains[layer_at, 0]).astype(jnp.bfloat16)
        gate_part = jnp.dot(normed, w_gate[layer_at], preferred_element_type=jnp.float32)
        up_part = jnp.dot(normed, w_up[layer_at], preferred_element_type=jnp.float32)
        activated = (jax.nn.gelu(gate_part, approximate=True) * up_part).astype(jnp.bfloat16)
        mlp_out = jnp.dot(activated, w_down[layer_at], preferred_element_type=jnp.float32)
        current = current + norm_rows(mlp_out, norm_gains[layer_at, 1])
        current_b = current.astype(jnp.bfloat16)
        ple_gate_out = jnp.dot(current_b, ple_gate[layer_at], preferred_element_type=jnp.float32)
        ple_act = (jax.nn.gelu(ple_gate_out, approximate=True) * ple_part[:, layer_at, :]).astype(jnp.bfloat16)
        ple_out = jnp.dot(ple_act, ple_proj[layer_at], preferred_element_type=jnp.float32)
        current = current + norm_rows(ple_out, norm_gains[layer_at, 2])
    return current.astype(jnp.bfloat16)
```

```python
import functools

import jax
import jax.numpy as jnp
from jax import lax
from jax.experimental import pallas as pl
from jax.experimental.pallas import tpu as pltpu
from jax.sharding import PartitionSpec as P


PLE = 256
CHUNKS = 2

epsilon = 1e-06


def gelu(v):
    return 0.5 * v * (1.0 + jnp.tanh(0.7978845608028654 * (v + 0.044715 * (v * v * v))))


def norm_rows(values, scales):
    return values * lax.rsqrt(jnp.mean(values * values, axis=-1, keepdims=True) + epsilon) * scales


def block_order(members):
    near = members.bit_length() - 3
    return sorted(range(members), key=lambda r: ([(r >> b) & 1 for b in range(near)], r))


def mlp_body(
    me, hidden, gains, w_gate, w_up, w_down, keep, send,
    rows, gate_w, up_w, down_w, act, result, in_sems, gate_sems, up_sems, down_sems, out_sems,
    *, order, first, count, parts,
):
    members = len(order)
    half = members // 2
    tiles, _, tile = gate_w.shape
    out_tiles, _, out_tile = down_w.shape

    def fetch(i):
        return pltpu.make_async_copy(
            hidden.at[order[i] ^ me[0], pl.ds(first, count), :], rows.at[i], in_sems.at[i]
        )

    def weights(j):
        return (
            pltpu.make_async_copy(w_gate.at[:, pl.ds(j * tile, tile)], gate_w.at[j], gate_sems.at[j]),
            pltpu.make_async_copy(w_up.at[:, pl.ds(j * tile, tile)], up_w.at[j], up_sems.at[j]),
        )

    def down(j):
        return pltpu.make_async_copy(w_down.at[:, pl.ds(j * out_tile, out_tile)], down_w.at[j], down_sems.at[j])

    def put(j, part):
        return pltpu.make_async_copy(
            result.at[j, pl.ds(part * half, half)],
            (keep, send)[part].at[:, :, pl.ds(j * out_tile, out_tile)],
            out_sems.at[j, part],
        )

    for i in range(members):
        fetch(i).start()
    for j in range(tiles):
        for copy in weights(j):
            copy.start()
    for j in range(out_tiles):
        down(j).start()
    for i in range(members):
        fetch(i).wait()
        rows[i] = norm_rows(rows[i].astype(jnp.float32), gains[...]).astype(jnp.bfloat16)
    per = members // parts
    size = per * count
    for j in range(tiles):
        for copy in weights(j):
            copy.wait()
        for part in range(parts):
            x = rows[part * per : (part + 1) * per].reshape(size, rows.shape[2])
            gate = jnp.dot(x, gate_w[j], preferred_element_type=jnp.float32)
            up = jnp.dot(x, up_w[j], preferred_element_type=jnp.float32)
            act[j, part * size : (part + 1) * size, :] = (gelu(gate) * up).astype(jnp.bfloat16)
    for j in range(out_tiles):
        down(j).wait()
        for part in range(parts):
            total = None
            for k in range(tiles):
                piece = jnp.dot(
                    act[k, part * size : (part + 1) * size, :],
                    down_w[j, k * tile : (k + 1) * tile, :],
                    preferred_element_type=jnp.float32,
                )
                total = piece if total is None else total + piece
            result[j, part * per : (part + 1) * per] = total.reshape(per, count, out_tile).astype(result.dtype)
        put(j, 0).start()
        put(j, 1).start()
    for j in range(out_tiles):
        put(j, 0).wait()
        put(j, 1).wait()


def mlp_chunk(me, hidden, gains, w_gate, w_up, w_down, chunk, count, tile=512, out_tile=512, parts=2):
    members, _, width = hidden.shape
    units = w_gate.shape[1]
    order = block_order(members)
    half = members // 2
    tile = min(tile, units)
    tiles = units // tile
    out_tile = min(out_tile, width)
    out_tiles = width // out_tile
    out = jax.ShapeDtypeStruct((half, count, width), jnp.bfloat16)
    anywhere = pl.BlockSpec(memory_space=pl.ANY)
    return pl.pallas_call(
        functools.partial(mlp_body, order=order, first=chunk * count, count=count, parts=parts),
        out_shape=(out, out),
        in_specs=[pl.BlockSpec(memory_space=pltpu.SMEM), anywhere, pl.BlockSpec(memory_space=pltpu.VMEM)] + [anywhere] * 3,
        out_specs=[anywhere, anywhere],
        scratch_shapes=[
            pltpu.VMEM((members, count, width), jnp.bfloat16),
            pltpu.VMEM((tiles, width, tile), jnp.bfloat16),
            pltpu.VMEM((tiles, width, tile), jnp.bfloat16),
            pltpu.VMEM((out_tiles, units, out_tile), jnp.bfloat16),
            pltpu.VMEM((tiles, members * count, tile), jnp.bfloat16),
            pltpu.VMEM((out_tiles, members, count, out_tile), jnp.bfloat16),
            pltpu.SemaphoreType.DMA((members,)),
            pltpu.SemaphoreType.DMA((tiles,)),
            pltpu.SemaphoreType.DMA((tiles,)),
            pltpu.SemaphoreType.DMA((out_tiles,)),
            pltpu.SemaphoreType.DMA((out_tiles, 2)),
        ],
        compiler_params=pltpu.CompilerParams(vmem_limit_bytes=48 << 20),
        cost_estimate=pl.CostEstimate(
            flops=6 * members * count * width * units,
            bytes_accessed=6 * width * units,
            transcendentals=members * count * units,
        ),
        name="mlp",
    )(me, hidden, gains, w_gate, w_up, w_down)


def ple_body(me, keep, recv, from_x, from_y, hidden, gains, looked, mine, mate, out, weights, sems, *, order):
    half, _, share, _ = mine.shape
    members = 2 * half

    def fetch(j, source):
        relative = j ^ me[0]
        place = sum(((relative >> bit) & 1) << i for i, bit in enumerate(order[:-1]))
        return pltpu.make_async_copy(
            source.at[place], weights.at[:, pl.ds(j * share, share), :], sems.at[j]
        )

    for j in range(members):
        other = ((j ^ me[0]) >> order[-1]) & 1

        @pl.when(other == 0)
        def _():
            fetch(j, mine).start()

        @pl.when(other == 1)
        def _():
            fetch(j, mate).start()

    f32 = jnp.float32
    branch = keep[0].astype(f32) + recv[0].astype(f32) + from_x[...].astype(f32) + from_y[...].astype(f32)
    current = hidden[0].astype(f32) + norm_rows(branch, gains[1:2, :])
    current_b = current.astype(jnp.bfloat16)
    for j in range(members):
        fetch(j, mine).wait()
    gate = lax.dot_general(current_b, weights[0], (((1,), (1,)), ((), ())), preferred_element_type=f32)
    act = (gelu(gate) * (looked[...].astype(f32) * PLE**0.5)).astype(jnp.bfloat16)
    branch = jnp.dot(act, weights[1], preferred_element_type=f32)
    out[...] = (current + norm_rows(branch, gains[2:3, :])).astype(out.dtype)


def ple_chunk(me, keep, recv, from_x, from_y, hidden, gains, looked, mine, mate, order, chunk, count):
    width = hidden.shape[2]
    half, _, share, _ = mine.shape
    members = 2 * half
    block = pl.BlockSpec((1, count, width), lambda i, me: (0, 0, 0))
    flat = pl.BlockSpec((count, width), lambda i, me: (0, 0))
    anywhere = pl.BlockSpec(memory_space=pl.ANY)
    return pl.pallas_call(
        functools.partial(ple_body, order=order),
        out_shape=jax.ShapeDtypeStruct((count, width), jnp.bfloat16),
        grid_spec=pltpu.PrefetchScalarGridSpec(
            num_scalar_prefetch=1,
            grid=(1,),
            in_specs=[
                block,
                block,
                flat,
                flat,
                pl.BlockSpec((1, count, width), lambda i, me: (me[0], chunk, 0)),
                pl.BlockSpec(gains.shape, lambda i, me: (0, 0)),
                pl.BlockSpec((count, looked.shape[1]), lambda i, me: (chunk, 0)),
                anywhere,
                anywhere,
            ],
            out_specs=flat,
            scratch_shapes=[
                pltpu.VMEM((2, members * share, width), jnp.bfloat16),
                pltpu.SemaphoreType.DMA((members,)),
            ],
        ),
        compiler_params=pltpu.CompilerParams(dimension_semantics=("arbitrary",), vmem_limit_bytes=48 << 20),
        cost_estimate=pl.CostEstimate(flops=4 * count * width * members * share, bytes_accessed=members * share * width * 4, transcendentals=count * members * share),
        name="ple",
    )(me, keep, recv, from_x, from_y, hidden, gains, looked, mine, mate)


def far_body(keep, recv, low, high):
    total = (keep[0].astype(jnp.float32) + recv[0].astype(jnp.float32)).astype(low.dtype)
    low[...] = total[:, : low.shape[1]]
    high[...] = total[:, low.shape[1] :]


def far_sum(keep, recv):
    _, count, width = keep.shape
    block = pl.BlockSpec((1, count, width), lambda i: (3, 0, 0))
    part = pl.BlockSpec((count, width // 2), lambda i: (0, 0))
    out = jax.ShapeDtypeStruct((count, width // 2), keep.dtype)
    return pl.pallas_call(
        far_body,
        out_shape=(out, out),
        grid=(1,),
        in_specs=[block, block],
        out_specs=[part, part],
        cost_estimate=pl.CostEstimate(flops=count * width, bytes_accessed=6 * count * width, transcendentals=0),
        name="far",
    )(keep, recv)


def side_body(keep_x, recv_x, keep_y, recv_y, low, high, to_x, to_y):
    f32 = jnp.float32
    part = pl.program_id(0)
    x = keep_x[0].astype(f32) + recv_x[0].astype(f32)
    y = keep_y[0].astype(f32) + recv_y[0].astype(f32)

    @pl.when(part == 0)
    def _():
        to_x[...] = x.astype(to_x.dtype)
        to_y[...] = (y + low[...].astype(f32)).astype(to_y.dtype)

    @pl.when(part == 1)
    def _():
        to_x[...] = (x + high[...].astype(f32)).astype(to_x.dtype)
        to_y[...] = y.astype(to_y.dtype)


def side_sum(keep, recv, low, high):
    _, count, width = keep.shape
    half = width // 2
    block_x = pl.BlockSpec((1, count, half), lambda i: (1, 0, i))
    block_y = pl.BlockSpec((1, count, half), lambda i: (2, 0, i))
    part = pl.BlockSpec((count, half), lambda i: (0, 0))
    side = pl.BlockSpec((count, half), lambda i: (0, i))
    out = jax.ShapeDtypeStruct((count, width), keep.dtype)
    return pl.pallas_call(
        side_body,
        out_shape=(out, out),
        grid=(2,),
        in_specs=[block_x, block_x, block_y, block_y, part, part],
        out_specs=[side, side],
        compiler_params=pltpu.CompilerParams(dimension_semantics=("arbitrary",)),
        cost_estimate=pl.CostEstimate(flops=3 * count * width, bytes_accessed=14 * count * width, transcendentals=0),
        name="side",
    )(keep, recv, keep, recv, low, high)


def place_body(me, *refs, plan, count, aliased):
    n = len(plan)
    pieces = refs[:n]
    out = refs[n + aliased]
    stage, sems_in, sems_out = refs[n + aliased + 1 :]

    def take(i):
        size = plan[i][2]
        return pltpu.make_async_copy(pieces[i], stage.at[i, :, pl.ds(0, size)], sems_in.at[i])

    def put(i):
        relative, low, size, chunk = plan[i]
        return pltpu.make_async_copy(
            stage.at[i, :, pl.ds(0, size)],
            out.at[relative ^ me[0], pl.ds(chunk * count, count), pl.ds(low, size)],
            sems_out.at[i],
        )

    for i in range(n):
        take(i).start()
    for i in range(n):
        take(i).wait()
        put(i).start()
    for i in range(n):
        put(i).wait()


def place(me, pieces, out, shape, count):
    plan = [(r, low, a.shape[1], chunk) for r, low, a, chunk in pieces]
    arrays = [p[2] for p in pieces]
    aliased = out is not None
    anywhere = pl.BlockSpec(memory_space=pl.ANY)
    return pl.pallas_call(
        functools.partial(place_body, plan=plan, count=count, aliased=int(aliased)),
        out_shape=jax.ShapeDtypeStruct(shape, jnp.bfloat16),
        in_specs=[pl.BlockSpec(memory_space=pltpu.SMEM)] + [anywhere] * (len(arrays) + aliased),
        out_specs=anywhere,
        scratch_shapes=[
            pltpu.VMEM((len(arrays), count, shape[2]), jnp.bfloat16),
            pltpu.SemaphoreType.DMA((len(arrays),)),
            pltpu.SemaphoreType.DMA((len(arrays),)),
        ],
        input_output_aliases={1 + len(arrays): 0} if aliased else {},
        name="place",
    )(me, *arrays, *([out] if aliased else []))


def after(value, *others):
    return lax.optimization_barrier((value,) + others)[0]


def ask(token_slab, token_row, slab_owner, devices, slots):
    tokens = token_row.shape[0]
    hit_slab = token_slab == jnp.arange(slab_owner.shape[0], dtype=jnp.int32)[None, :]
    target = jnp.sum(jnp.where(hit_slab, slab_owner[None, :], 0), axis=1)
    order = jnp.arange(tokens, dtype=jnp.int32)
    earlier = (target[None, :] == target[:, None]) & (order[None, :] < order[:, None])
    slot_of = jnp.sum(earlier.astype(jnp.int32), axis=1)
    place_of = target * slots + slot_of
    hit = place_of[:, None] == jnp.arange(devices * slots, dtype=jnp.int32)[None, :]
    requests = jnp.sum(jnp.where(hit, token_row[:, None], 0), axis=0).reshape(devices, slots)
    return place_of, jnp.pad(requests, ((0, 0), (0, -slots % 128)))


def per_device(
    hidden,
    token_slab,
    token_row,
    slab_owner,
    ple_table,
    norm_gains,
    w_gate,
    w_up,
    w_down,
    ple_gate,
    ple_proj,
):
    members = lax.axis_size("member")
    axes = ("group", "member")
    devices = lax.axis_size("group") * members
    bits = members.bit_length() - 1
    bx, by = bits - 2, bits - 1
    near = list(range(bits - 2))
    width = hidden.shape[1]
    low = width // 2
    tokens = token_row.shape[0]
    count = tokens // CHUNKS
    channels = ple_table.shape[1]
    slots = max(2, (2 * tokens + devices - 1) // devices)
    slots += -slots % 16
    f32, bf16 = jnp.float32, jnp.bfloat16
    me = lax.axis_index("member").astype(jnp.int32)[None]
    blocks = hidden.reshape(members, tokens, width)
    gains = norm_gains[0]

    def swap(v, bit):
        return lax.ppermute(v, "member", [(i, i ^ (1 << bit)) for i in range(members)])

    def feed(chunk, *deps):
        return mlp_chunk(after(me, *deps), blocks, gains[0:1], w_gate[0], w_up[0], w_down[0], chunk, count)

    def reduce_near(keep, send):
        recv = swap(send, near[0])
        for bit in near[1:]:
            both = (keep.astype(f32) + recv.astype(f32)).astype(bf16)
            keep, send = both[: both.shape[0] // 2], both[both.shape[0] // 2 :]
            recv = swap(send, bit)
        return keep, recv

    def far_swap(parts):
        return swap(parts[0], bx), swap(parts[1], by)

    def side_swap(parts):
        return swap(parts[0], bx), swap(parts[1], by)

    order = [by, bx] + near
    small = [jnp.stack([ple_gate[0].T, ple_proj[0]])[None]]

    def spread(i):
        small.append(swap(small[i], order[i]))
        if i + 1 < len(order):
            small[i + 1] = jnp.concatenate(small[i : i + 2], axis=0)

    place_of, requests = ask(token_slab, token_row, slab_owner, devices, slots)
    wanted = lax.all_to_all(requests, axes, 0, 0, tiled=True)[:, :slots]

    spread(0)
    half = [feed(0, requests)]
    half.append(feed(1, half[0][0], small[1]))
    spread(1)
    summed = [reduce_near(*half[0])]
    far_out = far_sum(*summed[0])
    far = far_swap(far_out)
    summed.append(reduce_near(*half[1]))
    served = jnp.take(ple_table, after(wanted, *far_out).reshape(-1), axis=0, mode="clip")
    side_out = side_sum(*summed[0], after(far[0], served), far[1])
    side = [side_swap(side_out)]
    far_out = far_sum(*summed[1])
    returned = lax.all_to_all(
        after(served, *side_out, *far_out).reshape(devices, slots, channels), axes, 0, 0, tiled=True
    )
    far = far_swap(far_out)
    for i in range(2, len(order)):
        spread(i)
    side.append(side_swap(side_sum(*summed[1], *far)))
    hit = place_of[:, None] == jnp.arange(devices * slots, dtype=jnp.int32)[None, :]
    looked = jnp.dot(
        hit.astype(bf16), returned.reshape(devices * slots, channels), preferred_element_type=f32
    ).astype(bf16)

    x, y = 1 << bx, 1 << by
    pieces = []
    for chunk in range(CHUNKS):
        own = ple_chunk(me, *summed[chunk], *side[chunk], blocks, gains, looked, *small[-2:], order, chunk, count)
        x_own = swap(own, bx)
        y_own = swap(own, by)
        early = [(0, 0, own), (x, 0, x_own), (y, 0, y_own)]
        late = [(x | y, 0, swap(y_own[:, :low], bx)), (x | y, low, swap(x_own[:, low:], by))]
        for group in (early, late):
            for bit in reversed(near):
                group = group + [(r | (1 << bit), start, swap(a, bit)) for r, start, a in group]
            pieces.append([p + (chunk,) for p in group])
    out = None
    for group in (pieces[0], pieces[1] + pieces[2], pieces[3]):
        out = place(me, group, out, blocks.shape, count)
    return out.reshape(hidden.shape)


def solution(mesh):
    return jax.shard_map(
        per_device,
        mesh=mesh,
        in_specs=(
            P("group", None),
            P(("group", "member"), None),
            P(("group", "member")),
            P(),
            P(("group", "member"), None),
            P(),
            P(None, None, "member"),
            P(None, None, "member"),
            P(None, "member", None),
            P(None, None, "member"),
            P(None, "member", None),
        ),
        out_specs=P("group", None),
        check_vma=False,
    )
```

```python
import functools

import jax
import jax.numpy as jnp
from jax import lax
from jax.experimental import pallas as pl
from jax.experimental.pallas import tpu as pltpu
from jax.sharding import PartitionSpec as P


PLE = 256
CHUNKS = 2

epsilon = 1e-06


def gelu(v):
    return 0.5 * v * (1.0 + jnp.tanh(0.7978845608028654 * (v + 0.044715 * (v * v * v))))


def norm_rows(values, scales):
    return values * lax.rsqrt(jnp.mean(values * values, axis=-1, keepdims=True) + epsilon) * scales


def block_order(members):
    near = members.bit_length() - 3
    return sorted(range(members), key=lambda r: ([(r >> b) & 1 for b in range(near)], r))


def mlp_body(
    me, hidden, gains, w_gate, w_up, w_down, keep, send,
    rows, gate_w, up_w, down_w, act, result, in_sems, gate_sems, up_sems, down_sems, out_sems,
    *, order, first, count, parts,
):
    members = len(order)
    half = members // 2
    tiles, _, tile = gate_w.shape
    out_tiles, _, out_tile = down_w.shape

    def fetch(i):
        return pltpu.make_async_copy(
            hidden.at[order[i] ^ me[0], pl.ds(first, count), :], rows.at[i], in_sems.at[i]
        )

    def weights(j):
        return (
            pltpu.make_async_copy(w_gate.at[:, pl.ds(j * tile, tile)], gate_w.at[j], gate_sems.at[j]),
            pltpu.make_async_copy(w_up.at[:, pl.ds(j * tile, tile)], up_w.at[j], up_sems.at[j]),
        )

    def down(j):
        return pltpu.make_async_copy(w_down.at[:, pl.ds(j * out_tile, out_tile)], down_w.at[j], down_sems.at[j])

    def put(j, part):
        return pltpu.make_async_copy(
            result.at[j, pl.ds(part * half, half)],
            (keep, send)[part].at[:, :, pl.ds(j * out_tile, out_tile)],
            out_sems.at[j, part],
        )

    for i in range(members):
        fetch(i).start()
    for j in range(tiles):
        for copy in weights(j):
            copy.start()
    for j in range(out_tiles):
        down(j).start()
    for i in range(members):
        fetch(i).wait()
        rows[i] = norm_rows(rows[i].astype(jnp.float32), gains[...]).astype(jnp.bfloat16)
    per = members // parts
    size = per * count
    for j in range(tiles):
        for copy in weights(j):
            copy.wait()
        for part in range(parts):
            x = rows[part * per : (part + 1) * per].reshape(size, rows.shape[2])
            gate = jnp.dot(x, gate_w[j], preferred_element_type=jnp.float32)
            up = jnp.dot(x, up_w[j], preferred_element_type=jnp.float32)
            act[j, part * size : (part + 1) * size, :] = (gelu(gate) * up).astype(jnp.bfloat16)
    for j in range(out_tiles):
        down(j).wait()
        for part in range(parts):
            total = None
            for k in range(tiles):
                piece = jnp.dot(
                    act[k, part * size : (part + 1) * size, :],
                    down_w[j, k * tile : (k + 1) * tile, :],
                    preferred_element_type=jnp.float32,
                )
                total = piece if total is None else total + piece
            result[j, part * per : (part + 1) * per] = total.reshape(per, count, out_tile).astype(result.dtype)
        put(j, 0).start()
        put(j, 1).start()
    for j in range(out_tiles):
        put(j, 0).wait()
        put(j, 1).wait()


def mlp_chunk(me, hidden, gains, w_gate, w_up, w_down, chunk, count, tile=512, out_tile=512, parts=2):
    members, _, width = hidden.shape
    units = w_gate.shape[1]
    order = block_order(members)
    half = members // 2
    tile = min(tile, units)
    tiles = units // tile
    out_tile = min(out_tile, width)
    out_tiles = width // out_tile
    out = jax.ShapeDtypeStruct((half, count, width), jnp.bfloat16)
    anywhere = pl.BlockSpec(memory_space=pl.ANY)
    return pl.pallas_call(
        functools.partial(mlp_body, order=order, first=chunk * count, count=count, parts=parts),
        out_shape=(out, out),
        in_specs=[pl.BlockSpec(memory_space=pltpu.SMEM), anywhere, pl.BlockSpec(memory_space=pltpu.VMEM)] + [anywhere] * 3,
        out_specs=[pl.BlockSpec(memory_space=pltpu.HBM)] * 2,
        scratch_shapes=[
            pltpu.VMEM((members, count, width), jnp.bfloat16),
            pltpu.VMEM((tiles, width, tile), jnp.bfloat16),
            pltpu.VMEM((tiles, width, tile), jnp.bfloat16),
            pltpu.VMEM((out_tiles, units, out_tile), jnp.bfloat16),
            pltpu.VMEM((tiles, members * count, tile), jnp.bfloat16),
            pltpu.VMEM((out_tiles, members, count, out_tile), jnp.bfloat16),
            pltpu.SemaphoreType.DMA((members,)),
            pltpu.SemaphoreType.DMA((tiles,)),
            pltpu.SemaphoreType.DMA((tiles,)),
            pltpu.SemaphoreType.DMA((out_tiles,)),
            pltpu.SemaphoreType.DMA((out_tiles, 2)),
        ],
        compiler_params=pltpu.CompilerParams(vmem_limit_bytes=48 << 20),
        cost_estimate=pl.CostEstimate(
            flops=6 * members * count * width * units,
            bytes_accessed=6 * width * units,
            transcendentals=members * count * units,
        ),
        name="mlp",
    )(me, hidden, gains, w_gate, w_up, w_down)


def ple_body(me, keep, recv, from_x, from_y, hidden, gains, looked, mine, mate, out, weights, sems, *, order):
    half, _, share, _ = mine.shape
    members = 2 * half

    def fetch(j, source):
        relative = j ^ me[0]
        place = sum(((relative >> bit) & 1) << i for i, bit in enumerate(order[:-1]))
        return pltpu.make_async_copy(
            source.at[place], weights.at[:, pl.ds(j * share, share), :], sems.at[j]
        )

    for j in range(members):
        other = ((j ^ me[0]) >> order[-1]) & 1

        @pl.when(other == 0)
        def _():
            fetch(j, mine).start()

        @pl.when(other == 1)
        def _():
            fetch(j, mate).start()

    f32 = jnp.float32
    branch = keep[0].astype(f32) + recv[0].astype(f32) + from_x[...].astype(f32) + from_y[...].astype(f32)
    current = hidden[0].astype(f32) + norm_rows(branch, gains[1:2, :])
    current_b = current.astype(jnp.bfloat16)
    for j in range(members):
        fetch(j, mine).wait()
    gate = lax.dot_general(current_b, weights[0], (((1,), (1,)), ((), ())), preferred_element_type=f32)
    act = (gelu(gate) * (looked[...].astype(f32) * PLE**0.5)).astype(jnp.bfloat16)
    branch = jnp.dot(act, weights[1], preferred_element_type=f32)
    out[...] = (current + norm_rows(branch, gains[2:3, :])).astype(out.dtype)


def ple_chunk(me, keep, recv, from_x, from_y, hidden, gains, looked, mine, mate, order, chunk, count):
    width = hidden.shape[2]
    half, _, share, _ = mine.shape
    members = 2 * half
    block = pl.BlockSpec((1, count, width), lambda i, me: (0, 0, 0))
    flat = pl.BlockSpec((count, width), lambda i, me: (0, 0))
    anywhere = pl.BlockSpec(memory_space=pl.ANY)
    return pl.pallas_call(
        functools.partial(ple_body, order=order),
        out_shape=jax.ShapeDtypeStruct((count, width), jnp.bfloat16),
        grid_spec=pltpu.PrefetchScalarGridSpec(
            num_scalar_prefetch=1,
            grid=(1,),
            in_specs=[
                block,
                block,
                flat,
                flat,
                pl.BlockSpec((1, count, width), lambda i, me: (me[0], chunk, 0)),
                pl.BlockSpec(gains.shape, lambda i, me: (0, 0)),
                pl.BlockSpec((count, looked.shape[1]), lambda i, me: (chunk, 0)),
                anywhere,
                anywhere,
            ],
            out_specs=flat,
            scratch_shapes=[
                pltpu.VMEM((2, members * share, width), jnp.bfloat16),
                pltpu.SemaphoreType.DMA((members,)),
            ],
        ),
        compiler_params=pltpu.CompilerParams(dimension_semantics=("arbitrary",), vmem_limit_bytes=48 << 20),
        cost_estimate=pl.CostEstimate(flops=4 * count * width * members * share, bytes_accessed=members * share * width * 4, transcendentals=count * members * share),
        name="ple",
    )(me, keep, recv, from_x, from_y, hidden, gains, looked, mine, mate)


def far_body(keep, recv, low, high):
    total = (keep[0].astype(jnp.float32) + recv[0].astype(jnp.float32)).astype(low.dtype)
    low[...] = total[:, : low.shape[1]]
    high[...] = total[:, low.shape[1] :]


def far_sum(keep, recv):
    _, count, width = keep.shape
    block = pl.BlockSpec((1, count, width), lambda i: (3, 0, 0))
    part = pl.BlockSpec((count, width // 2), lambda i: (0, 0))
    out = jax.ShapeDtypeStruct((count, width // 2), keep.dtype)
    return pl.pallas_call(
        far_body,
        out_shape=(out, out),
        grid=(1,),
        in_specs=[block, block],
        out_specs=[part, part],
        cost_estimate=pl.CostEstimate(flops=count * width, bytes_accessed=6 * count * width, transcendentals=0),
        name="far",
    )(keep, recv)


def side_body(keep_x, recv_x, keep_y, recv_y, low, high, to_x, to_y):
    f32 = jnp.float32
    part = pl.program_id(0)
    x = keep_x[0].astype(f32) + recv_x[0].astype(f32)
    y = keep_y[0].astype(f32) + recv_y[0].astype(f32)

    @pl.when(part == 0)
    def _():
        to_x[...] = x.astype(to_x.dtype)
        to_y[...] = (y + low[...].astype(f32)).astype(to_y.dtype)

    @pl.when(part == 1)
    def _():
        to_x[...] = (x + high[...].astype(f32)).astype(to_x.dtype)
        to_y[...] = y.astype(to_y.dtype)


def side_sum(keep, recv, low, high):
    _, count, width = keep.shape
    half = width // 2
    block_x = pl.BlockSpec((1, count, half), lambda i: (1, 0, i))
    block_y = pl.BlockSpec((1, count, half), lambda i: (2, 0, i))
    part = pl.BlockSpec((count, half), lambda i: (0, 0))
    side = pl.BlockSpec((count, half), lambda i: (0, i))
    out = jax.ShapeDtypeStruct((count, width), keep.dtype)
    return pl.pallas_call(
        side_body,
        out_shape=(out, out),
        grid=(2,),
        in_specs=[block_x, block_x, block_y, block_y, part, part],
        out_specs=[side, side],
        compiler_params=pltpu.CompilerParams(dimension_semantics=("arbitrary",)),
        cost_estimate=pl.CostEstimate(flops=3 * count * width, bytes_accessed=14 * count * width, transcendentals=0),
        name="side",
    )(keep, recv, keep, recv, low, high)


def place_body(me, *refs, plan, count, aliased):
    n = len(plan)
    pieces = refs[:n]
    out = refs[n + aliased]
    stage, sems_in, sems_out = refs[n + aliased + 1 :]

    def take(i):
        size = plan[i][2]
        return pltpu.make_async_copy(pieces[i], stage.at[i, :, pl.ds(0, size)], sems_in.at[i])

    def put(i):
        relative, low, size, chunk = plan[i]
        return pltpu.make_async_copy(
            stage.at[i, :, pl.ds(0, size)],
            out.at[relative ^ me[0], pl.ds(chunk * count, count), pl.ds(low, size)],
            sems_out.at[i],
        )

    for i in range(n):
        take(i).start()
    for i in range(n):
        take(i).wait()
        put(i).start()
    for i in range(n):
        put(i).wait()


def place(me, pieces, out, shape, count):
    plan = [(r, low, a.shape[1], chunk) for r, low, a, chunk in pieces]
    arrays = [p[2] for p in pieces]
    aliased = out is not None
    anywhere = pl.BlockSpec(memory_space=pl.ANY)
    return pl.pallas_call(
        functools.partial(place_body, plan=plan, count=count, aliased=int(aliased)),
        out_shape=jax.ShapeDtypeStruct(shape, jnp.bfloat16),
        in_specs=[pl.BlockSpec(memory_space=pltpu.SMEM)] + [anywhere] * (len(arrays) + aliased),
        out_specs=anywhere,
        scratch_shapes=[
            pltpu.VMEM((len(arrays), count, shape[2]), jnp.bfloat16),
            pltpu.SemaphoreType.DMA((len(arrays),)),
            pltpu.SemaphoreType.DMA((len(arrays),)),
        ],
        input_output_aliases={1 + len(arrays): 0} if aliased else {},
        name="place",
    )(me, *arrays, *([out] if aliased else []))


def after(value, *others):
    return lax.optimization_barrier((value,) + others)[0]


def ask(token_slab, token_row, slab_owner, devices, slots):
    tokens = token_row.shape[0]
    hit_slab = token_slab == jnp.arange(slab_owner.shape[0], dtype=jnp.int32)[None, :]
    target = jnp.sum(jnp.where(hit_slab, slab_owner[None, :], 0), axis=1)
    order = jnp.arange(tokens, dtype=jnp.int32)
    earlier = (target[None, :] == target[:, None]) & (order[None, :] < order[:, None])
    slot_of = jnp.sum(earlier.astype(jnp.int32), axis=1)
    place_of = target * slots + slot_of
    hit = place_of[:, None] == jnp.arange(devices * slots, dtype=jnp.int32)[None, :]
    requests = jnp.sum(jnp.where(hit, token_row[:, None], 0), axis=0).reshape(devices, slots)
    return place_of, jnp.pad(requests, ((0, 0), (0, -slots % 128)))


def per_device(
    hidden,
    token_slab,
    token_row,
    slab_owner,
    ple_table,
    norm_gains,
    w_gate,
    w_up,
    w_down,
    ple_gate,
    ple_proj,
):
    members = lax.axis_size("member")
    axes = ("group", "member")
    devices = lax.axis_size("group") * members
    bits = members.bit_length() - 1
    bx, by = bits - 2, bits - 1
    near = list(range(bits - 2))
    width = hidden.shape[1]
    low = width // 2
    tokens = token_row.shape[0]
    count = tokens // CHUNKS
    channels = ple_table.shape[1]
    slots = max(2, (2 * tokens + devices - 1) // devices)
    slots += -slots % 16
    f32, bf16 = jnp.float32, jnp.bfloat16
    me = lax.axis_index("member").astype(jnp.int32)[None]
    blocks = hidden.reshape(members, tokens, width)
    gains = norm_gains[0]

    def swap(v, bit):
        return lax.ppermute(v, "member", [(i, i ^ (1 << bit)) for i in range(members)])

    def feed(chunk, *deps):
        return mlp_chunk(after(me, *deps), blocks, gains[0:1], w_gate[0], w_up[0], w_down[0], chunk, count)

    def reduce_near(keep, send):
        recv = swap(send, near[0])
        for bit in near[1:]:
            both = (keep.astype(f32) + recv.astype(f32)).astype(bf16)
            keep, send = both[: both.shape[0] // 2], both[both.shape[0] // 2 :]
            recv = swap(send, bit)
        return keep, recv

    def far_swap(parts):
        return swap(parts[0], bx), swap(parts[1], by)

    def side_swap(parts):
        return swap(parts[0], bx), swap(parts[1], by)

    order = [by, bx] + near
    small = [jnp.stack([ple_gate[0].T, ple_proj[0]])[None]]

    def spread(i):
        small.append(swap(small[i], order[i]))
        if i + 1 < len(order):
            small[i + 1] = jnp.concatenate(small[i : i + 2], axis=0)

    place_of, requests = ask(token_slab, token_row, slab_owner, devices, slots)
    wanted = lax.all_to_all(requests, axes, 0, 0, tiled=True)[:, :slots]

    spread(0)
    half = [feed(0, requests)]
    served = jnp.take(ple_table, after(wanted, half[0][0]).reshape(-1), axis=0, mode="clip")
    returned = lax.all_to_all(served.reshape(devices, slots, channels), axes, 0, 0, tiled=True)
    half.append(feed(1, half[0][0], small[1], served))
    spread(1)
    summed = [reduce_near(*half[chunk]) for chunk in range(CHUNKS)]
    far_out = [far_sum(*summed[chunk]) for chunk in range(CHUNKS)]
    far = [far_swap(far_out[chunk]) for chunk in range(CHUNKS)]
    for i in range(2, len(order)):
        spread(i)
    side = [side_swap(side_sum(*summed[chunk], *far[chunk])) for chunk in range(CHUNKS)]
    hit = place_of[:, None] == jnp.arange(devices * slots, dtype=jnp.int32)[None, :]
    looked = jnp.dot(
        hit.astype(bf16), returned.reshape(devices * slots, channels), preferred_element_type=f32
    ).astype(bf16)

    x, y = 1 << bx, 1 << by
    pieces = []
    for chunk in range(CHUNKS):
        own = ple_chunk(me, *summed[chunk], *side[chunk], blocks, gains, looked, *small[-2:], order, chunk, count)
        x_own = swap(own, bx)
        y_own = swap(own, by)
        early = [(0, 0, own), (x, 0, x_own), (y, 0, y_own)]
        late = [(x | y, 0, swap(y_own[:, :low], bx)), (x | y, low, swap(x_own[:, low:], by))]
        for group in (early, late):
            for bit in reversed(near):
                group = group + [(r | (1 << bit), start, swap(a, bit)) for r, start, a in group]
            pieces.append([p + (chunk,) for p in group])
    out = None
    for group in (pieces[0], pieces[1] + pieces[2], pieces[3]):
        out = place(me, group, out, blocks.shape, count)
    return out.reshape(hidden.shape)


def solution(mesh):
    return jax.shard_map(
        per_device,
        mesh=mesh,
        in_specs=(
            P("group", None),
            P(("group", "member"), None),
            P(("group", "member")),
            P(),
            P(("group", "member"), None),
            P(),
            P(None, None, "member"),
            P(None, None, "member"),
            P(None, "member", None),
            P(None, None, "member"),
            P(None, "member", None),
        ),
        out_specs=P("group", None),
        check_vma=False,
    )
```

```python
import functools

import jax
import jax.numpy as jnp
from jax import lax
from jax.experimental import pallas as pl
from jax.experimental.pallas import tpu as pltpu
from jax.sharding import PartitionSpec as P


PLE = 256
CHUNKS = 2

epsilon = 1e-06


def gelu(v):
    return 0.5 * v * (1.0 + jnp.tanh(0.7978845608028654 * (v + 0.044715 * (v * v * v))))


def norm_rows(values, scales):
    return values * lax.rsqrt(jnp.mean(values * values, axis=-1, keepdims=True) + epsilon) * scales


def block_order(members):
    near = members.bit_length() - 3
    return sorted(range(members), key=lambda r: ([(r >> b) & 1 for b in range(near)], r))


def mlp_body(
    me, hidden, gains, w_gate, w_up, w_down, keep, send,
    rows, gate_w, up_w, down_w, act, result, in_sems, gate_sems, up_sems, down_sems, out_sems,
    *, order, first, count, parts,
):
    members = len(order)
    half = members // 2
    tiles, _, tile = gate_w.shape
    out_tiles, _, out_tile = down_w.shape

    def fetch(i):
        return pltpu.make_async_copy(
            hidden.at[order[i] ^ me[0], pl.ds(first, count), :], rows.at[i], in_sems.at[i]
        )

    def weights(j):
        return (
            pltpu.make_async_copy(w_gate.at[:, pl.ds(j * tile, tile)], gate_w.at[j], gate_sems.at[j]),
            pltpu.make_async_copy(w_up.at[:, pl.ds(j * tile, tile)], up_w.at[j], up_sems.at[j]),
        )

    def down(j):
        return pltpu.make_async_copy(w_down.at[:, pl.ds(j * out_tile, out_tile)], down_w.at[j], down_sems.at[j])

    def put(j, part):
        return pltpu.make_async_copy(
            result.at[j, pl.ds(part * half, half)],
            (keep, send)[part].at[:, :, pl.ds(j * out_tile, out_tile)],
            out_sems.at[j, part],
        )

    for i in range(members):
        fetch(i).start()
    for copy in weights(0):
        copy.start()
    for i in range(members):
        fetch(i).wait()
        rows[i] = norm_rows(rows[i].astype(jnp.float32), gains[...]).astype(jnp.bfloat16)
    per = members // parts
    size = per * count
    for j in range(tiles):
        for copy in weights(j):
            copy.wait()
        if j == 0:
            for later in range(1, tiles):
                for copy in weights(later):
                    copy.start()
            for later in range(out_tiles):
                down(later).start()
        for part in range(parts):
            x = rows[part * per : (part + 1) * per].reshape(size, rows.shape[2])
            gate = jnp.dot(x, gate_w[j], preferred_element_type=jnp.float32)
            up = jnp.dot(x, up_w[j], preferred_element_type=jnp.float32)
            act[j, part * size : (part + 1) * size, :] = (gelu(gate) * up).astype(jnp.bfloat16)
    for j in range(out_tiles):
        down(j).wait()
        for part in range(parts):
            total = None
            for k in range(tiles):
                piece = jnp.dot(
                    act[k, part * size : (part + 1) * size, :],
                    down_w[j, k * tile : (k + 1) * tile, :],
                    preferred_element_type=jnp.float32,
                )
                total = piece if total is None else total + piece
            result[j, part * per : (part + 1) * per] = total.reshape(per, count, out_tile).astype(result.dtype)
        put(j, 0).start()
        put(j, 1).start()
    for j in range(out_tiles):
        put(j, 0).wait()
        put(j, 1).wait()


def mlp_chunk(me, hidden, gains, w_gate, w_up, w_down, chunk, count, tile=512, out_tile=512, parts=2):
    members, _, width = hidden.shape
    units = w_gate.shape[1]
    order = block_order(members)
    half = members // 2
    tile = min(tile, units)
    tiles = units // tile
    out_tile = min(out_tile, width)
    out_tiles = width // out_tile
    out = jax.ShapeDtypeStruct((half, count, width), jnp.bfloat16)
    anywhere = pl.BlockSpec(memory_space=pl.ANY)
    return pl.pallas_call(
        functools.partial(mlp_body, order=order, first=chunk * count, count=count, parts=parts),
        out_shape=(out, out),
        in_specs=[pl.BlockSpec(memory_space=pltpu.SMEM), anywhere, pl.BlockSpec(memory_space=pltpu.VMEM)] + [anywhere] * 3,
        out_specs=[pl.BlockSpec(memory_space=pltpu.HBM)] * 2,
        scratch_shapes=[
            pltpu.VMEM((members, count, width), jnp.bfloat16),
            pltpu.VMEM((tiles, width, tile), jnp.bfloat16),
            pltpu.VMEM((tiles, width, tile), jnp.bfloat16),
            pltpu.VMEM((out_tiles, units, out_tile), jnp.bfloat16),
            pltpu.VMEM((tiles, members * count, tile), jnp.bfloat16),
            pltpu.VMEM((out_tiles, members, count, out_tile), jnp.bfloat16),
            pltpu.SemaphoreType.DMA((members,)),
            pltpu.SemaphoreType.DMA((tiles,)),
            pltpu.SemaphoreType.DMA((tiles,)),
            pltpu.SemaphoreType.DMA((out_tiles,)),
            pltpu.SemaphoreType.DMA((out_tiles, 2)),
        ],
        compiler_params=pltpu.CompilerParams(vmem_limit_bytes=48 << 20),
        cost_estimate=pl.CostEstimate(
            flops=6 * members * count * width * units,
            bytes_accessed=6 * width * units,
            transcendentals=members * count * units,
        ),
        name="mlp",
    )(me, hidden, gains, w_gate, w_up, w_down)


def ple_body(me, keep, recv, from_x, from_y, hidden, gains, looked, mine, mate, out, weights, sems, *, order):
    half, _, share, _ = mine.shape
    members = 2 * half

    def fetch(j, source):
        relative = j ^ me[0]
        place = sum(((relative >> bit) & 1) << i for i, bit in enumerate(order[:-1]))
        return pltpu.make_async_copy(
            source.at[place], weights.at[:, pl.ds(j * share, share), :], sems.at[j]
        )

    for j in range(members):
        other = ((j ^ me[0]) >> order[-1]) & 1

        @pl.when(other == 0)
        def _():
            fetch(j, mine).start()

        @pl.when(other == 1)
        def _():
            fetch(j, mate).start()

    f32 = jnp.float32
    branch = keep[0].astype(f32) + recv[0].astype(f32) + from_x[...].astype(f32) + from_y[...].astype(f32)
    current = hidden[0].astype(f32) + norm_rows(branch, gains[1:2, :])
    current_b = current.astype(jnp.bfloat16)
    for j in range(members):
        fetch(j, mine).wait()
    gate = lax.dot_general(current_b, weights[0], (((1,), (1,)), ((), ())), preferred_element_type=f32)
    act = (gelu(gate) * (looked[...].astype(f32) * PLE**0.5)).astype(jnp.bfloat16)
    branch = jnp.dot(act, weights[1], preferred_element_type=f32)
    out[...] = (current + norm_rows(branch, gains[2:3, :])).astype(out.dtype)


def ple_chunk(me, keep, recv, from_x, from_y, hidden, gains, looked, mine, mate, order, chunk, count):
    width = hidden.shape[2]
    half, _, share, _ = mine.shape
    members = 2 * half
    block = pl.BlockSpec((1, count, width), lambda i, me: (0, 0, 0))
    flat = pl.BlockSpec((count, width), lambda i, me: (0, 0))
    anywhere = pl.BlockSpec(memory_space=pl.ANY)
    return pl.pallas_call(
        functools.partial(ple_body, order=order),
        out_shape=jax.ShapeDtypeStruct((count, width), jnp.bfloat16),
        grid_spec=pltpu.PrefetchScalarGridSpec(
            num_scalar_prefetch=1,
            grid=(1,),
            in_specs=[
                block,
                block,
                flat,
                flat,
                pl.BlockSpec((1, count, width), lambda i, me: (me[0], chunk, 0)),
                pl.BlockSpec(gains.shape, lambda i, me: (0, 0)),
                pl.BlockSpec((count, looked.shape[1]), lambda i, me: (chunk, 0)),
                anywhere,
                anywhere,
            ],
            out_specs=flat,
            scratch_shapes=[
                pltpu.VMEM((2, members * share, width), jnp.bfloat16),
                pltpu.SemaphoreType.DMA((members,)),
            ],
        ),
        compiler_params=pltpu.CompilerParams(dimension_semantics=("arbitrary",), vmem_limit_bytes=48 << 20),
        cost_estimate=pl.CostEstimate(flops=4 * count * width * members * share, bytes_accessed=members * share * width * 4, transcendentals=count * members * share),
        name="ple",
    )(me, keep, recv, from_x, from_y, hidden, gains, looked, mine, mate)


def far_body(keep, recv, low, high):
    total = (keep[0].astype(jnp.float32) + recv[0].astype(jnp.float32)).astype(low.dtype)
    low[...] = total[:, : low.shape[1]]
    high[...] = total[:, low.shape[1] :]


def far_sum(keep, recv):
    _, count, width = keep.shape
    block = pl.BlockSpec((1, count, width), lambda i: (3, 0, 0))
    part = pl.BlockSpec((count, width // 2), lambda i: (0, 0))
    out = jax.ShapeDtypeStruct((count, width // 2), keep.dtype)
    return pl.pallas_call(
        far_body,
        out_shape=(out, out),
        grid=(1,),
        in_specs=[block, block],
        out_specs=[part, part],
        cost_estimate=pl.CostEstimate(flops=count * width, bytes_accessed=6 * count * width, transcendentals=0),
        name="far",
    )(keep, recv)


def side_body(keep_x, recv_x, keep_y, recv_y, low, high, to_x, to_y):
    f32 = jnp.float32
    part = pl.program_id(0)
    x = keep_x[0].astype(f32) + recv_x[0].astype(f32)
    y = keep_y[0].astype(f32) + recv_y[0].astype(f32)

    @pl.when(part == 0)
    def _():
        to_x[...] = x.astype(to_x.dtype)
        to_y[...] = (y + low[...].astype(f32)).astype(to_y.dtype)

    @pl.when(part == 1)
    def _():
        to_x[...] = (x + high[...].astype(f32)).astype(to_x.dtype)
        to_y[...] = y.astype(to_y.dtype)


def side_sum(keep, recv, low, high):
    _, count, width = keep.shape
    half = width // 2
    block_x = pl.BlockSpec((1, count, half), lambda i: (1, 0, i))
    block_y = pl.BlockSpec((1, count, half), lambda i: (2, 0, i))
    part = pl.BlockSpec((count, half), lambda i: (0, 0))
    side = pl.BlockSpec((count, half), lambda i: (0, i))
    out = jax.ShapeDtypeStruct((count, width), keep.dtype)
    return pl.pallas_call(
        side_body,
        out_shape=(out, out),
        grid=(2,),
        in_specs=[block_x, block_x, block_y, block_y, part, part],
        out_specs=[side, side],
        compiler_params=pltpu.CompilerParams(dimension_semantics=("arbitrary",)),
        cost_estimate=pl.CostEstimate(flops=3 * count * width, bytes_accessed=14 * count * width, transcendentals=0),
        name="side",
    )(keep, recv, keep, recv, low, high)


def place_body(me, *refs, plan, count, aliased):
    n = len(plan)
    pieces = refs[:n]
    out = refs[n + aliased]
    stage, sems_in, sems_out = refs[n + aliased + 1 :]

    def take(i):
        size = plan[i][2]
        return pltpu.make_async_copy(pieces[i], stage.at[i, :, pl.ds(0, size)], sems_in.at[i])

    def put(i):
        relative, low, size, chunk = plan[i]
        return pltpu.make_async_copy(
            stage.at[i, :, pl.ds(0, size)],
            out.at[relative ^ me[0], pl.ds(chunk * count, count), pl.ds(low, size)],
            sems_out.at[i],
        )

    for i in range(n):
        take(i).start()
    for i in range(n):
        take(i).wait()
        put(i).start()
    for i in range(n):
        put(i).wait()


def place(me, pieces, out, shape, count):
    plan = [(r, low, a.shape[1], chunk) for r, low, a, chunk in pieces]
    arrays = [p[2] for p in pieces]
    aliased = out is not None
    anywhere = pl.BlockSpec(memory_space=pl.ANY)
    return pl.pallas_call(
        functools.partial(place_body, plan=plan, count=count, aliased=int(aliased)),
        out_shape=jax.ShapeDtypeStruct(shape, jnp.bfloat16),
        in_specs=[pl.BlockSpec(memory_space=pltpu.SMEM)] + [anywhere] * (len(arrays) + aliased),
        out_specs=anywhere,
        scratch_shapes=[
            pltpu.VMEM((len(arrays), count, shape[2]), jnp.bfloat16),
            pltpu.SemaphoreType.DMA((len(arrays),)),
            pltpu.SemaphoreType.DMA((len(arrays),)),
        ],
        input_output_aliases={1 + len(arrays): 0} if aliased else {},
        name="place",
    )(me, *arrays, *([out] if aliased else []))


def after(value, *others):
    return lax.optimization_barrier((value,) + others)[0]


def ask(token_slab, token_row, slab_owner, devices, slots):
    tokens = token_row.shape[0]
    hit_slab = token_slab == jnp.arange(slab_owner.shape[0], dtype=jnp.int32)[None, :]
    target = jnp.sum(jnp.where(hit_slab, slab_owner[None, :], 0), axis=1)
    order = jnp.arange(tokens, dtype=jnp.int32)
    earlier = (target[None, :] == target[:, None]) & (order[None, :] < order[:, None])
    slot_of = jnp.sum(earlier.astype(jnp.int32), axis=1)
    place_of = target * slots + slot_of
    hit = place_of[:, None] == jnp.arange(devices * slots, dtype=jnp.int32)[None, :]
    requests = jnp.sum(jnp.where(hit, token_row[:, None], 0), axis=0).reshape(devices, slots)
    return place_of, jnp.pad(requests, ((0, 0), (0, -slots % 128)))


def per_device(
    hidden,
    token_slab,
    token_row,
    slab_owner,
    ple_table,
    norm_gains,
    w_gate,
    w_up,
    w_down,
    ple_gate,
    ple_proj,
):
    members = lax.axis_size("member")
    axes = ("group", "member")
    devices = lax.axis_size("group") * members
    bits = members.bit_length() - 1
    bx, by = bits - 2, bits - 1
    near = list(range(bits - 2))
    width = hidden.shape[1]
    low = width // 2
    tokens = token_row.shape[0]
    count = tokens // CHUNKS
    channels = ple_table.shape[1]
    slots = max(2, (2 * tokens + devices - 1) // devices)
    slots += -slots % 16
    f32, bf16 = jnp.float32, jnp.bfloat16
    me = lax.axis_index("member").astype(jnp.int32)[None]
    blocks = hidden.reshape(members, tokens, width)
    gains = norm_gains[0]

    def swap(v, bit):
        return lax.ppermute(v, "member", [(i, i ^ (1 << bit)) for i in range(members)])

    def feed(chunk, *deps):
        return mlp_chunk(after(me, *deps), blocks, gains[0:1], w_gate[0], w_up[0], w_down[0], chunk, count)

    def reduce_near(keep, send):
        recv = swap(send, near[0])
        for bit in near[1:]:
            both = (keep.astype(f32) + recv.astype(f32)).astype(bf16)
            keep, send = both[: both.shape[0] // 2], both[both.shape[0] // 2 :]
            recv = swap(send, bit)
        return keep, recv

    def far_swap(parts):
        return swap(parts[0], bx), swap(parts[1], by)

    def side_swap(parts):
        return swap(parts[0], bx), swap(parts[1], by)

    order = [by, bx] + near
    small = [jnp.stack([ple_gate[0].T, ple_proj[0]])[None]]

    def spread(i):
        small.append(swap(small[i], order[i]))
        if i + 1 < len(order):
            small[i + 1] = jnp.concatenate(small[i : i + 2], axis=0)

    place_of, requests = ask(token_slab, token_row, slab_owner, devices, slots)
    wanted = lax.all_to_all(requests, axes, 0, 0, tiled=True)[:, :slots]

    spread(0)
    half = [feed(0, requests)]
    served = jnp.take(ple_table, after(wanted, half[0][0]).reshape(-1), axis=0, mode="clip")
    returned = lax.all_to_all(served.reshape(devices, slots, channels), axes, 0, 0, tiled=True)
    half.append(feed(1, half[0][0], small[1], served))
    spread(1)
    summed = [reduce_near(*half[chunk]) for chunk in range(CHUNKS)]
    far_out = [far_sum(*summed[chunk]) for chunk in range(CHUNKS)]
    far = [far_swap(far_out[chunk]) for chunk in range(CHUNKS)]
    for i in range(2, len(order)):
        spread(i)
    side = [side_swap(side_sum(*summed[chunk], *far[chunk])) for chunk in range(CHUNKS)]
    hit = place_of[:, None] == jnp.arange(devices * slots, dtype=jnp.int32)[None, :]
    looked = jnp.dot(
        hit.astype(bf16), returned.reshape(devices * slots, channels), preferred_element_type=f32
    ).astype(bf16)

    x, y = 1 << bx, 1 << by
    pieces = []
    for chunk in range(CHUNKS):
        own = ple_chunk(me, *summed[chunk], *side[chunk], blocks, gains, looked, *small[-2:], order, chunk, count)
        x_own = swap(own, bx)
        y_own = swap(own, by)
        early = [(0, 0, own), (x, 0, x_own), (y, 0, y_own)]
        late = [(x | y, 0, swap(y_own[:, :low], bx)), (x | y, low, swap(x_own[:, low:], by))]
        for group in (early, late):
            for bit in reversed(near):
                group = group + [(r | (1 << bit), start, swap(a, bit)) for r, start, a in group]
            pieces.append([p + (chunk,) for p in group])
    out = None
    for group in (pieces[0], pieces[1] + pieces[2], pieces[3]):
        out = place(me, group, out, blocks.shape, count)
    return out.reshape(hidden.shape)


def solution(mesh):
    return jax.shard_map(
        per_device,
        mesh=mesh,
        in_specs=(
            P("group", None),
            P(("group", "member"), None),
            P(("group", "member")),
            P(),
            P(("group", "member"), None),
            P(),
            P(None, None, "member"),
            P(None, None, "member"),
            P(None, "member", None),
            P(None, None, "member"),
            P(None, "member", None),
        ),
        out_specs=P("group", None),
        check_vma=False,
    )
```
